128 devices in a mesh: data: 1, dap2: 16 (over z, y), dap: 8 (over x, core).
Axes of the slice: x: 4, y: 4, z: 4, core: 2. Of those that a mesh axis runs over, the one named last changes fastest.
Arguments:
- pair_act: float32 [384, 384, 128], P(('data', 'dap'), 'dap2')
- pair_mask: int32 [384, 384], P(('data', 'dap'), 'dap2')
- ln_z: bfloat16 [16, 2, 2, 128], replicated
- w_ab: bfloat16 [16, 2, 128, 512], replicated
- w_g: bfloat16 [16, 2, 128, 128], replicated
- ln_x: bfloat16 [16, 2, 2, 128], replicated
- w_o: bfloat16 [16, 2, 128, 128], replicated
Outputs:
- output: float32 [384, 384, 128], P(('data', 'dap'), 'dap2')
All inputs are finite; a program needn't handle non-finite values.
Results may differ from the reference program's by a relative error of at most 0.00408477.
Values are sent between devices in bfloat16 or wider.
A program may use at most 1 GiB of HBM per device.

```python
import jax
import jax.numpy as jnp
from jax import lax

N_RES = 384
C_Z = 128
C_HID = 128
LAYERS = 16
ROW_BLOCK = 64
LN_EPS = 1e-5


def norm_params(base_key, width):
    key_gain, key_bias = jax.random.split(base_key)
    gain = 1.0 + 0.3 * jax.random.normal(key_gain, (LAYERS, 2, 1, width), jnp.float32)
    bias = 0.3 * jax.random.normal(key_bias, (LAYERS, 2, 1, width), jnp.float32)
    return jnp.concatenate([gain, bias], axis=2).astype(jnp.bfloat16)


def setup_inputs(seed: int = 0, part: int = 0) -> dict:
    part_key = jax.random.fold_in(jax.random.key(seed), part)
    key_act, key_len, key_hole = jax.random.split(part_key, 3)
    key_lnz, key_ab, key_gate, key_lnx, key_out = jax.random.split(jax.random.key(seed + 1), 5)
    pair_act = jax.random.normal(key_act, (N_RES, N_RES, C_Z), jnp.float32)
    valid_len = jax.random.randint(key_len, (), N_RES - N_RES // 8, N_RES - N_RES // 16 + 1)
    hole_draw = jax.random.randint(key_hole, (N_RES, N_RES), 0, 32)
    inside = jnp.arange(N_RES) < valid_len
    pair_mask = (inside[:, None] & inside[None, :] & (hole_draw != 0)).astype(jnp.int32)
    w_ab = (jax.random.normal(key_ab, (LAYERS, 2, C_Z, 4 * C_HID), jnp.float32) * C_Z ** -0.5).astype(jnp.bfloat16)
    w_g = (jax.random.normal(key_gate, (LAYERS, 2, C_Z, C_Z), jnp.float32) * C_Z ** -0.5).astype(jnp.bfloat16)
    w_o = (jax.random.normal(key_out, (LAYERS, 2, C_HID, C_Z), jnp.float32) * (C_HID * LAYERS) ** -0.5).astype(jnp.bfloat16)
    return {"pair_act": pair_act, "pair_mask": pair_mask, "ln_z": norm_params(key_lnz, C_Z), "w_ab": w_ab, "w_g": w_g, "ln_x": norm_params(key_lnx, C_HID), "w_o": w_o}


def layer_norm(values, params):
    mean = jnp.mean(values, axis=-1, keepdims=True)
    centered = values - mean
    variance = jnp.mean(centered * centered, axis=-1, keepdims=True)
    scaled = centered * lax.rsqrt(variance + LN_EPS)
    return (scaled * params[0].astype(jnp.float32) + params[1].astype(jnp.float32)).astype(jnp.bfloat16)


def project_rows(z_rows, mask_rows, ln_params, w_ab):
    z_norm = layer_norm(z_rows, ln_params)
    projected = jnp.dot(z_norm.reshape(-1, C_Z), w_ab, preferred_element_type=jnp.float32).reshape(ROW_BLOCK, N_RES, 4 * C_HID)
    keep_mask = mask_rows.astype(jnp.float32)[:, :, None]
    a_proj = (keep_mask * jax.nn.sigmoid(projected[:, :, C_HID:2 * C_HID]) * projected[:, :, :C_HID]).astype(jnp.bfloat16)
    b_proj = (keep_mask * jax.nn.sigmoid(projected[:, :, 3 * C_HID:]) * projected[:, :, 2 * C_HID:3 * C_HID]).astype(jnp.bfloat16)
    return a_proj, b_proj


def tri_update(pair_state, pair_mask, ln_z, w_ab, w_g, ln_x, w_o, outgoing):
    n_blocks = N_RES // ROW_BLOCK
    z_blocks = pair_state.reshape(n_blocks, ROW_BLOCK, N_RES, C_Z)
    mask_blocks = pair_mask.reshape(n_blocks, ROW_BLOCK, N_RES)

    def project_block(block_pair):
        return project_rows(block_pair[0], block_pair[1], ln_z, w_ab)

    a_all, b_all = lax.map(project_block, (z_blocks, mask_blocks))
    a_all = a_all.reshape(N_RES, N_RES, C_HID)
    b_all = b_all.reshape(N_RES, N_RES, C_HID)
    if not outgoing:
        a_all = jnp.swapaxes(a_all, 0, 1)
        b_all = jnp.swapaxes(b_all, 0, 1)
    b_wide = b_all.astype(jnp.float32)

    def finish_block(block_pair):
        z_rows, a_rows = block_pair
        x_sum = jnp.einsum("ikc,jkc->ijc", a_rows.astype(jnp.float32), b_wide)
        x_norm = layer_norm(x_sum, ln_x)
        update_val = jnp.dot(x_norm.reshape(-1, C_HID), w_o, preferred_element_type=jnp.float32).reshape(ROW_BLOCK, N_RES, C_Z)
        z_norm = layer_norm(z_rows, ln_z)
        gate_val = jax.nn.sigmoid(jnp.dot(z_norm.reshape(-1, C_Z), w_g, preferred_element_type=jnp.float32)).reshape(ROW_BLOCK, N_RES, C_Z)
        return z_rows + gate_val * update_val

    new_blocks = lax.map(finish_block, (z_blocks, a_all.reshape(n_blocks, ROW_BLOCK, N_RES, C_HID)))
    return new_blocks.reshape(N_RES, N_RES, C_Z)


def reference(pair_act, pair_mask, ln_z, w_ab, w_g, ln_x, w_o):
    def one_layer(pair_state, layer_params):
        ln_z_layer, w_ab_layer, w_g_layer, ln_x_layer, w_o_layer = layer_params
        pair_state = tri_update(pair_state, pair_mask, ln_z_layer[0], w_ab_layer[0], w_g_layer[0], ln_x_layer[0], w_o_layer[0], True)
        pair_state = tri_update(pair_state, pair_mask, ln_z_layer[1], w_ab_layer[1], w_g_layer[1], ln_x_layer[1], w_o_layer[1], False)
        return pair_state, None

    pair_out, _ = lax.scan(one_layer, pair_act, (ln_z, w_ab, w_g, ln_x, w_o))
    return pair_out
```

```python
import functools

import jax
import jax.numpy as jnp
from jax import lax
from jax.experimental import pallas as pl
from jax.experimental.pallas import tpu as pltpu
from jax.sharding import PartitionSpec as P

LN_EPS = 1e-5
N_DEV = 128
CH = 128
N = 384
R = 3
MESH = pl.DeviceIdType.MESH


def norm_cols(v, gain, bias):
    mean = jnp.mean(v, axis=0, keepdims=True)
    cen = v - mean
    var = jnp.mean(cen * cen, axis=0, keepdims=True)
    return (cen * lax.rsqrt(var + LN_EPS) * gain + bias).astype(jnp.bfloat16)


def body(n_layers, z_in, mask, w_in, w_out, lnp, z_ref,
         s_ab, r_ab, s_x, r_x, stage, stage2, a_mat, b_mat, xn_buf,
         sem_sab, sem_rab, sem_sx, sem_rx):
    d2 = lax.axis_index("dap2")
    d1 = lax.axis_index("dap")
    cz, cy = d2 // 4, d2 % 4
    cx, cc = d1 // 2, d1 % 2
    me = d1 * 16 + d2
    cols = [((cx + dx) % 4) * 2 + (cc + dc) % 2 for dx in (2, 1, 3, 0) for dc in (1, 0)]

    def all_peers(fn):
        def one(q, carry):
            dz, dy = (4 - q // 4 + 3) % 4, (4 - q % 4 + 3) % 4
            t2 = ((cz + dz) % 4) * 4 + (cy + dy) % 4
            for i, t1 in enumerate(cols):
                if i == 7:
                    @pl.when(q != 15)
                    def _():
                        fn(t2, t1)
                else:
                    fn(t2, t1)
            return carry
        lax.fori_loop(0, 16, one, 0)

    bar = pltpu.get_barrier_semaphore()
    all_peers(lambda t2, t1: pl.semaphore_signal(bar, inc=1, device_id=(0, t2, t1), device_id_type=MESH))
    pl.semaphore_wait(bar, N_DEV - 1)

    z_ref[...] = z_in[...]

    def send(src, dst, rows, sem_s, sem_r, r):
        def one(t2, t1):
            t = t1 * 16 + t2
            pltpu.make_async_remote_copy(
                src_ref=src.at[r, pl.ds(t * rows, rows)], dst_ref=dst.at[r, pl.ds(me * rows, rows)],
                send_sem=sem_s.at[r], recv_sem=sem_r.at[r], device_id=(0, t2, t1), device_id_type=MESH).start()
        all_peers(one)

    def wait(src, dst, rows, sem, r):
        part = pl.ds(0, rows * (N_DEV - 1))
        pltpu.make_async_copy(src.at[r, part], dst.at[r, part], sem.at[r]).wait()

    def project(u, r, first):
        tok = pl.ds(r * N, N)
        zn = norm_cols(z_ref[:, tok], lnp[u, :, 0:1], lnp[u, :, 1:2])
        q = jnp.dot(w_in[u], zn, preferred_element_type=jnp.float32)
        m = mask[:, tok]
        a = m * jax.nn.sigmoid(q[CH:2 * CH]) * q[:CH]
        b = m * jax.nn.sigmoid(q[3 * CH:4 * CH]) * q[2 * CH:3 * CH]
        xn_buf[:, tok] = jax.nn.sigmoid(q[4 * CH:])
        for kh in range(3):
            stage[pl.ds(2 * kh, CH, stride=6), :] = a[:, kh * 128:(kh + 1) * 128]
            stage[pl.ds(2 * kh + 1, CH, stride=6), :] = b[:, kh * 128:(kh + 1) * 128]
        if not first:
            wait(s_ab, r_ab, 6, sem_sab, r)
        s_ab[r] = stage[...].astype(jnp.bfloat16)
        send(s_ab, r_ab, 6, sem_sab, sem_rab, r)

    def gather_mats(r):
        wait(s_ab, r_ab, 6, sem_rab, r)
        stage[...] = r_ab[r].astype(jnp.float32)
        stage2[...] = s_ab[r].astype(jnp.float32)
        stage[pl.ds(6 * me, 6), :] = stage2[pl.ds(6 * me, 6), :]
        for kh in range(3):
            a_mat[r * 128:(r + 1) * 128, kh * 128:(kh + 1) * 128] = stage[pl.ds(2 * kh, 128, stride=6), :].astype(jnp.bfloat16)
            b_mat[r * 128:(r + 1) * 128, kh * 128:(kh + 1) * 128] = stage[pl.ds(2 * kh + 1, 128, stride=6), :].astype(jnp.bfloat16)

    def contract(outgoing, r):
        if outgoing:
            x = lax.dot_general(a_mat[r * 128:(r + 1) * 128, :], b_mat[...], (((1,), (1,)), ((), ())),
                                preferred_element_type=jnp.float32)
        else:
            x = lax.dot_general(a_mat[:, r * 128:(r + 1) * 128], b_mat[...], (((0,), (0,)), ((), ())),
                                preferred_element_type=jnp.float32)
        for jh in range(3):
            s_x[r, pl.ds(jh, 128, stride=3), :] = x[:, jh * 128:(jh + 1) * 128]
        send(s_x, r_x, 3, sem_sx, sem_rx, r)

    def finish(u, r):
        wait(s_x, r_x, 3, sem_rx, r)
        r_x[r, pl.ds(3 * me, 3), :] = s_x[r, pl.ds(3 * me, 3), :]
        for jh in range(3):
            tok = slice(r * N + jh * 128, r * N + (jh + 1) * 128)
            x = r_x[r, pl.ds(jh, CH, stride=3), :]
            xn = norm_cols(x, lnp[u, :, 2:3], lnp[u, :, 3:4])
            y = jnp.dot(w_out[u], xn, preferred_element_type=jnp.float32)
            z_ref[:, tok] = z_ref[:, tok] + xn_buf[:, tok] * y
        wait(s_x, r_x, 3, sem_sx, r)

    def update(u, outgoing):
        for r in range(R):
            gather_mats(r)
        for r in range(R):
            contract(outgoing, r)
        for r in range(R):
            finish(u, r)

    for r in range(R):
        project(0, r, True)

    def layer(l, carry):
        update(2 * l, True)
        for r in range(R):
            project(2 * l + 1, r, False)
        update(2 * l + 1, False)

        @pl.when(l < n_layers - 1)
        def _():
            for r in range(R):
                project(2 * l + 2, r, False)
        return carry

    lax.fori_loop(0, n_layers, layer, 0)
    for r in range(R):
        wait(s_ab, r_ab, 6, sem_sab, r)


def solution(mesh):
    pair_spec = P(("data", "dap"), "dap2", None)
    mask_spec = P(("data", "dap"), "dap2")

    def local_stack(pair_act, pair_mask, ln_z, w_ab, w_g, ln_x, w_o):
        n_layers = w_o.shape[0]
        z = lax.all_to_all(pair_act, "dap2", 0, 1, tiled=True)
        z = z.reshape(R, N_DEV, R, CH).transpose(3, 0, 2, 1).reshape(CH, R * N)
        m = lax.all_to_all(pair_mask, "dap2", 0, 1, tiled=True)
        m = m.reshape(R, N_DEV, R).transpose(0, 2, 1).reshape(1, R * N).astype(jnp.float32)
        w_in = jnp.concatenate([w_ab, w_g], axis=-1).transpose(0, 1, 3, 2).reshape(2 * n_layers, 5 * CH, CH)
        w_out = w_o.transpose(0, 1, 3, 2).reshape(2 * n_layers, CH, CH)
        lnp = jnp.stack([ln_z[:, :, 0], ln_z[:, :, 1], ln_x[:, :, 0], ln_x[:, :, 1]], axis=-1)
        lnp = lnp.astype(jnp.float32).reshape(2 * n_layers, CH, 4)
        vmem = pl.BlockSpec(memory_space=pltpu.VMEM)
        dma = pltpu.SemaphoreType.DMA((R,))
        z = pl.pallas_call(
            functools.partial(body, n_layers),
            out_shape=jax.ShapeDtypeStruct((CH, R * N), jnp.float32),
            in_specs=[vmem] * 5, out_specs=vmem,
            scratch_shapes=[
                pltpu.VMEM((R, 6 * N_DEV, 128), jnp.bfloat16), pltpu.VMEM((R, 6 * N_DEV, 128), jnp.bfloat16),
                pltpu.VMEM((R, 3 * N_DEV, 128), jnp.float32), pltpu.VMEM((R, 3 * N_DEV, 128), jnp.float32),
                pltpu.VMEM((6 * N_DEV, 128), jnp.float32), pltpu.VMEM((6 * N_DEV, 128), jnp.float32),
                pltpu.VMEM((N, N), jnp.bfloat16), pltpu.VMEM((N, N), jnp.bfloat16),
                pltpu.VMEM((CH, R * N), jnp.float32), dma, dma, dma, dma],
            compiler_params=pltpu.CompilerParams(collective_id=0, has_side_effects=True, vmem_limit_bytes=56 * 2 ** 20),
            name="tri_stack",
        )(z, m, w_in, w_out, lnp)
        z = z.reshape(CH, R, R, N_DEV).transpose(1, 3, 2, 0).reshape(R, N, CH)
        return lax.all_to_all(z, "dap2", 1, 0, tiled=True)

    return jax.shard_map(local_stack, mesh=mesh, in_specs=(pair_spec, mask_spec, P(), P(), P(), P(), P()), out_specs=pair_spec, check_vma=False)
```

```python
import functools

import jax
import jax.numpy as jnp
from jax import lax
from jax.experimental import pallas as pl
from jax.experimental.pallas import tpu as pltpu
from jax.sharding import PartitionSpec as P

LN_EPS = 1e-5
N_DEV = 128
CH = 128
N = 384
R = 3
ROWS, COLS = 48, 24
CHUNKS = ((0, 1), (1, 1), (2, 1))
OFFSETS = sorted(((z, y, x, c) for z in (2, 1, 3, 0) for y in (2, 1, 3, 0) for x in (2, 1, 3, 0) for c in (1, 0) if z or y or x or c),
                 key=lambda o: -sum(min(v, 4 - v) for v in o[:3]))


def norm_cols(v, gain, bias):
    mean = jnp.mean(v, axis=0, keepdims=True)
    cen = v - mean
    var = jnp.mean(cen * cen, axis=0, keepdims=True)
    return (cen * lax.rsqrt(var + LN_EPS) * gain + bias).astype(jnp.bfloat16)


def wide(block):
    return jnp.concatenate([block] * 3, axis=1)


def body(n_layers, z_in, m_in, w_ab, w_g, w_o, ln_z, ln_x, z_out,
         zt, zrow, z_blk, mflat, mrow, mask, s_ab, r_ab, s_x, r_x, own_ab, stage, a_mat, b_mat, zn, gate,
         wab_raw, wg_raw, wo_raw, lnz_raw, lnx_raw, w_in, w_out, lnz, lnx,
         sem_sab, sem_rab, sem_sx, sem_rx, sem_w, sem_i, sem_s0, sem_r0, sem_s1, sem_r1, sem_s2, sem_r2):
    d2 = lax.axis_index("dap2")
    d1 = lax.axis_index("dap")
    cz, cy = d2 // 4, d2 % 4
    cx, cc = d1 // 2, d1 % 2
    me = d2 * 8 + d1
    zs, ys = [((cz + d) % 4) * 32 for d in range(4)], [((cy + d) % 4) * 8 for d in range(4)]
    xs = [[((cx + d) % 4) * 2 + (cc + e) % 2 for e in range(2)] for d in range(4)]
    peers = [zs[dz] + ys[dy] + xs[dx][dc] for dz, dy, dx, dc in OFFSETS]

    def dev(t):
        return dict(device_id=t, device_id_type=pl.DeviceIdType.LOGICAL)

    def fetches(u):
        return [pltpu.make_async_copy(src.at[u], dst, sem_w.at[k])
                for k, (src, dst) in enumerate(((w_ab, wab_raw), (w_g, wg_raw), (w_o, wo_raw)))]

    def fetch(u):
        for c in fetches(u):
            c.start()

    def prepare(u, slot):
        for c in fetches(u):
            c.wait()
        w_in[:4 * CH] = wab_raw[...].T
        w_in[4 * CH:] = wg_raw[...].T
        w_out[slot] = wo_raw[...].T
        for k in range(2):
            lnz[k] = jnp.broadcast_to(lnz_raw[u][k:k + 1].astype(jnp.float32), (CH, CH)).T
            lnx[slot, k] = jnp.broadcast_to(lnx_raw[u][k:k + 1].astype(jnp.float32), (CH, CH)).T

    fetch(0)
    firsts = [pltpu.make_async_copy(src, dst, sem_i.at[k])
              for k, (src, dst) in enumerate(((z_in, z_blk), (ln_z, lnz_raw), (ln_x, lnx_raw)))]
    for c in firsts:
        c.start()
    bar = pltpu.get_barrier_semaphore()
    for t in peers:
        pl.semaphore_signal(bar, inc=1, **dev(t))

    my_cols = pl.ds(pl.multiple_of(COLS * d2, 8), COLS)
    my_mask = pl.ds(3 * d2, 3)
    pad = jnp.concatenate([m_in[...].astype(jnp.float32), jnp.zeros((ROWS, N - COLS), jnp.float32)], axis=1)
    pad = pltpu.roll(pad, COLS * d2, 1)
    for t in range(3):
        mflat[pl.ds(t, ROWS, stride=3), :] = pad[:, t * 128:(t + 1) * 128]
    for c in firsts:
        c.wait()
    prepare(0, 0)
    pl.semaphore_wait(bar, N_DEV - 1)

    def block_rows(fn):
        def one(k, carry):
            ii = (k + R * d2) % ROWS
            i = ROWS * d1 + ii
            fn(ii, i % N_DEV, i // N_DEV)
            return carry
        lax.fori_loop(0, ROWS, one, 0)

    def move(src, dst, sem_s, sem_r, t):
        @pl.when(t == me)
        def _():
            dst[...] = src[...]

        @pl.when(t != me)
        def _():
            pltpu.make_async_remote_copy(src_ref=src, dst_ref=dst, send_sem=sem_s, recv_sem=sem_r, **dev(t)).start()

    def take(ref, unit, count, sem, but_one):
        for n, when in ((count - 1, but_one), (count, jnp.logical_not(but_one))):
            @pl.when(when)
            def _():
                some = ref.at[pl.ds(0, n * unit)]
                pltpu.make_async_copy(some, some, sem).wait()

    stays = (me + N_DEV * R - ROWS * d1) % N_DEV < ROWS

    def scatter(ii, g, r):
        move(z_blk.at[ii], zrow.at[r, my_cols], sem_s0, sem_r0.at[r], g)
        move(mflat.at[pl.ds(3 * ii, 3)], mrow.at[r, my_mask], sem_s1, sem_r1.at[r], g)

    block_rows(scatter)

    def toks(r):
        return pl.ds(pl.multiple_of(r * N, 128), N)

    def load_state(r):
        own = (me + N_DEV * r) // ROWS == d1
        take(zrow.at[r], COLS, 16, sem_r0.at[r], own)
        take(mrow.at[r], 3, 16, sem_r1.at[r], own)
        zt[:, toks(r)] = zrow[r].T
        for t in range(3):
            mask[r, :, t * 128:(t + 1) * 128] = jnp.sum(mrow[r, pl.ds(t, 16, stride=3), :], axis=0, keepdims=True)

    def part(ref, c, rows):
        r0, n = CHUNKS[c]
        return ref.at[r0, rows] if n == 1 else ref.at[pl.ds(r0, n), rows]

    def send(src, dst, rows, sem_s, sem_r, c):
        mine = part(dst, c, pl.ds(me * rows, rows))
        for t in peers:
            pltpu.make_async_remote_copy(src_ref=part(src, c, pl.ds(t * rows, rows)), dst_ref=mine,
                                         send_sem=sem_s.at[c], recv_sem=sem_r.at[c], **dev(t)).start()

    def wait(src, dst, rows, sem, c):
        most = pl.ds(0, rows * (N_DEV - 1))
        pltpu.make_async_copy(part(src, c, most), part(dst, c, most), sem.at[c]).wait()

    def rows_of(c, fn):
        r0, n = CHUNKS[c]
        if n == 1:
            fn(r0)
        else:
            def one(k, carry):
                fn(r0 + k)
                return carry
            lax.fori_loop(0, n, one, 0)

    def project(r):
        n = norm_cols(zt[:, toks(r)], wide(lnz[0]), wide(lnz[1]))
        zn[:, toks(r)] = n
        q = jnp.dot(w_in[:4 * CH], n, preferred_element_type=jnp.float32)
        m = mask[r]
        a = m * jax.nn.sigmoid(q[CH:2 * CH]) * q[:CH]
        b = m * jax.nn.sigmoid(q[3 * CH:]) * q[2 * CH:3 * CH]
        for kh in range(3):
            stage[pl.ds(2 * kh, CH, stride=6), :] = a[:, kh * 128:(kh + 1) * 128]
            stage[pl.ds(2 * kh + 1, CH, stride=6), :] = b[:, kh * 128:(kh + 1) * 128]
        own_ab[r, 0:6] = stage[pl.ds(6 * me, 6), :].astype(jnp.bfloat16).astype(jnp.float32)
        s_ab[r] = stage[...].astype(jnp.bfloat16)

    def gates():
        def one(r, carry):
            gate[:, toks(r)] = jax.nn.sigmoid(jnp.dot(w_in[4 * CH:], zn[:, toks(r)], preferred_element_type=jnp.float32))
            return carry
        lax.fori_loop(0, R, one, 0)

    def gather_mats(r):
        stage[...] = r_ab[r].astype(jnp.float32)
        stage[pl.ds(6 * me, 6), :] = own_ab[r, 0:6]
        row = pl.ds(pl.multiple_of(r * 128, 128), 128)
        for kh in range(3):
            a_mat[row, kh * 128:(kh + 1) * 128] = stage[pl.ds(2 * kh, 128, stride=6), :].astype(jnp.bfloat16)
            b_mat[row, kh * 128:(kh + 1) * 128] = stage[pl.ds(2 * kh + 1, 128, stride=6), :].astype(jnp.bfloat16)

    def contract(outgoing, r):
        row = pl.ds(pl.multiple_of(r * 128, 128), 128)
        if outgoing:
            x = lax.dot_general(a_mat[row, :], b_mat[...], (((1,), (1,)), ((), ())), preferred_element_type=jnp.float32)
        else:
            x = lax.dot_general(a_mat[:, row], b_mat[...], (((0,), (0,)), ((), ())), preferred_element_type=jnp.float32)
        for jh in range(3):
            s_x[r, pl.ds(jh, 128, stride=3), :] = x[:, jh * 128:(jh + 1) * 128]

    def finish(slot, r):
        r_x[r, pl.ds(3 * me, 3), :] = s_x[r, pl.ds(3 * me, 3), :]
        x = jnp.concatenate([r_x[r, pl.ds(jh, CH, stride=3), :] for jh in range(3)], axis=1)
        xn = norm_cols(x, wide(lnx[slot, 0]), wide(lnx[slot, 1]))
        y = jnp.dot(w_out[slot], xn, preferred_element_type=jnp.float32)
        zt[:, toks(r)] = zt[:, toks(r)] + gate[:, toks(r)] * y

    def leave(r):
        zrow[r] = zt[:, toks(r)].T
        i = me + N_DEV * r
        for k in range(16):
            b = (d2 + k) % 16
            move(zrow.at[r, pl.ds(pl.multiple_of(b * COLS, 8), COLS)], z_out.at[i % ROWS], sem_s2, sem_r2, b * 8 + i // ROWS)

    n_chunks = len(CHUNKS)

    def spread(outgoing):
        for c in range(n_chunks):
            wait(s_ab, r_ab, 6, sem_rab, c)
            rows_of(c, gather_mats)
        for c in range(n_chunks):
            rows_of(c, lambda r: contract(outgoing, r))
            send(s_x, r_x, 3, sem_sx, sem_rx, c)

    def collect(slot, c):
        wait(s_x, r_x, 3, sem_rx, c)
        rows_of(c, lambda r: finish(slot, r))
        wait(s_x, r_x, 3, sem_sx, c)

    def emit(c, first):
        if not first:
            wait(s_ab, r_ab, 6, sem_sab, c)
        rows_of(c, project)
        send(s_ab, r_ab, 6, sem_sab, sem_rab, c)

    for c in range(n_chunks):
        rows_of(c, load_state)
        emit(c, True)
    gates()

    take(z_blk, 1, ROWS, sem_s0, stays)
    take(mflat, 3, ROWS, sem_s1, stays)

    def layer(l, carry):
        fetch(2 * l + 1)
        spread(True)
        prepare(2 * l + 1, 1)
        for c in range(n_chunks):
            collect(0, c)
            emit(c, False)
        gates()
        more = l < n_layers - 1

        @pl.when(more)
        def _():
            fetch(2 * l + 2)
        spread(False)

        @pl.when(more)
        def _():
            prepare(2 * l + 2, 0)
        for c in range(n_chunks):
            collect(1, c)

            @pl.when(more)
            def _():
                emit(c, False)

            @pl.when(l == n_layers - 1)
            def _():
                rows_of(c, leave)

        @pl.when(more)
        def _():
            gates()
        return carry

    lax.fori_loop(0, n_layers, layer, 0)
    for c in range(n_chunks):
        wait(s_ab, r_ab, 6, sem_sab, c)

    take(z_out, 1, ROWS, sem_s2, stays)
    take(z_out, 1, ROWS, sem_r2, stays)


def solution(mesh):
    pair_spec = P(("data", "dap"), "dap2", None)
    mask_spec = P(("data", "dap"), "dap2")

    def local_stack(pair_act, pair_mask, ln_z, w_ab, w_g, ln_x, w_o):
        n_layers = w_o.shape[0]
        run_layers = n_layers
        vmem, hbm = pl.BlockSpec(memory_space=pltpu.VMEM), pl.BlockSpec(memory_space=pltpu.HBM)
        f32, bf16 = jnp.float32, jnp.bfloat16
        dma, dmas = pltpu.SemaphoreType.DMA, pltpu.SemaphoreType.DMA((R,))
        scratch = [
            ((CH, R * N), f32), ((R, N, CH), f32), (pair_act.shape, f32), ((R * ROWS, 128), f32), ((R, 3 * 16, 128), f32), ((R, 1, N), f32),
            ((R, 6 * N_DEV, 128), bf16), ((R, 6 * N_DEV, 128), bf16), ((R, 3 * N_DEV, 128), f32), ((R, 3 * N_DEV, 128), f32),
            ((R, 8, 128), f32), ((6 * N_DEV, 128), f32), ((N, N), bf16), ((N, N), bf16), ((CH, R * N), bf16), ((CH, R * N), f32),
            ((CH, 4 * CH), bf16), ((CH, CH), bf16), ((CH, CH), bf16), ((2 * n_layers, 2, CH), bf16), ((2 * n_layers, 2, CH), bf16), ((5 * CH, CH), bf16), ((2, CH, CH), bf16),
            ((2, CH, CH), f32), ((2, 2, CH, CH), f32)]
        return pl.pallas_call(
            functools.partial(body, run_layers),
            out_shape=jax.ShapeDtypeStruct(pair_act.shape, f32),
            in_specs=[hbm, vmem, hbm, hbm, hbm, hbm, hbm], out_specs=vmem,
            scratch_shapes=[pltpu.VMEM(s, t) for s, t in scratch] + [dmas] * 6 + [dma, dmas, dma, dmas, dma, dma],
            compiler_params=pltpu.CompilerParams(collective_id=0, has_side_effects=True, vmem_limit_bytes=67043328 - 800 * 1024),
            name="tri_stack",
        )(pair_act, pair_mask, w_ab.reshape(2 * n_layers, CH, 4 * CH), w_g.reshape(2 * n_layers, CH, CH),
          w_o.reshape(2 * n_layers, CH, CH), ln_z.reshape(2 * n_layers, 2, CH), ln_x.reshape(2 * n_layers, 2, CH))

    return jax.shard_map(local_stack, mesh=mesh, in_specs=(pair_spec, mask_spec, P(), P(), P(), P(), P()), out_specs=pair_spec, check_vma=False)
```
